32 devices in a mesh: grp: 2 (over x), tm: 16 (over z, y, core).
Axes of the slice: x: 2, y: 2, z: 4, core: 2. Of those that a mesh axis runs over, the one named last changes fastest.
Arguments:
- samples: bfloat16 [16, 2097152], P('grp', 'tm'), parts along dimension 0, may hold values from -128 to 127, as said below
- filter_taps: bfloat16 [16, 8192], replicated, may hold values from -4 to 4
Outputs:
- channelized: bfloat16 [16, 2, 4096, 256], P('grp', None, 'tm'), parts along dimension 0
The draws below stay inside these ranges and needn't reach their ends.
There are 2 independent parts, one for each index of `grp`. The reference program is written for one: setup_inputs(seed, part) draws one part's arguments, and reference() takes and returns one part's arrays. A program takes and returns all parts, laid end to end along the dimension named above; an argument that names none is the same for every part. Nothing has to cross between parts.
Inputs may be any that keep to these rules, and one draw needn't show every extreme that they name: `samples`: every sample is a whole number, as from an 8-bit converter.
All inputs are finite; a program needn't handle non-finite values.
Results may differ from the reference program's by a relative error of at most 0.007.
Values may be sent and summed in bfloat16 or wider, within the bound.
A program may use at most 128 MiB of HBM per device.

```python
import jax
import jax.numpy as jnp
from jax import lax

CHANNELS = 4096
FFT_LEN = 8192
ROW_LEN = 128
TAPS = 16
STREAMS = 8
SAMPLES = 2097152


def draw_samples(key, part):
    first_key, second_key = jax.random.split(jax.random.fold_in(key, 7))
    frame_total = SAMPLES // FFT_LEN
    base_level = jax.random.randint(first_key, (STREAMS, 1), 10, 61, dtype=jnp.int32)
    frame_index = (jnp.arange(SAMPLES, dtype=jnp.int32) // FFT_LEN)[None, :]
    amplitude = base_level * (frame_total + 2 * frame_index) // frame_total
    raw_bits = jax.random.randint(second_key, (STREAMS, SAMPLES), 0, 1048576, dtype=jnp.int32)
    values = raw_bits % (2 * amplitude + 1) - amplitude
    return jnp.clip(values, -128, 127).astype(jnp.bfloat16)


def scatter_about(key, extent, scale, bound, held_as=jnp.bfloat16):
    return jnp.clip(scale * jax.random.normal(key, extent, jnp.float32), -bound, bound).astype(held_as)


def setup_inputs(seed: int = 0, part: int = 0) -> dict:
    keys = jax.random.split(jax.random.key(seed), 3)
    part_keys = jax.random.split(jax.random.fold_in(keys[2], part), 3)
    samples = draw_samples(jax.random.fold_in(jax.random.fold_in(keys[2], part), 71), part)
    filter_taps = scatter_about(keys[1], (TAPS, FFT_LEN), 1.0, 4.0)
    return {"samples": samples, "filter_taps": filter_taps}


target_level = 0.378
epsilon = 1e-06

def tables(row_len, col_len):
    fft_len = row_len * col_len
    rows_a = jnp.arange(row_len, dtype=jnp.int32)
    cols_b = jnp.arange(col_len, dtype=jnp.int32)
    half_c = jnp.arange(col_len // 2, dtype=jnp.int32)
    angle_a = 2.0 * jnp.pi / row_len * (rows_a[:, None] * rows_a[None, :] % row_len).astype(jnp.float32)
    angle_t = 2.0 * jnp.pi / fft_len * (cols_b[:, None] * rows_a[None, :] % fft_len).astype(jnp.float32)
    angle_b = 2.0 * jnp.pi / col_len * (cols_b[:, None] * half_c[None, :] % col_len).astype(jnp.float32)
    return (jnp.cos(angle_a).astype(jnp.bfloat16), jnp.sin(angle_a).astype(jnp.bfloat16), jnp.cos(angle_t), jnp.sin(angle_t), jnp.cos(angle_b).astype(jnp.bfloat16), jnp.sin(angle_b).astype(jnp.bfloat16))

def transform(filtered):
    streams, frames, fft_len = filtered.shape
    col_len = fft_len // ROW_LEN
    cos_a, sin_a, cos_t, sin_t, cos_b, sin_b = tables(ROW_LEN, col_len)
    blocks = filtered.reshape(streams, frames, ROW_LEN, col_len).astype(jnp.float32)
    first_re = jnp.einsum('sfab,ad->sfbd', blocks, cos_a.astype(jnp.float32))
    first_im = -jnp.einsum('sfab,ad->sfbd', blocks, sin_a.astype(jnp.float32))
    twisted_re = lax.optimization_barrier((first_re * cos_t + first_im * sin_t).astype(jnp.bfloat16)).astype(jnp.float32)
    twisted_im = lax.optimization_barrier((first_im * cos_t - first_re * sin_t).astype(jnp.bfloat16)).astype(jnp.float32)
    cos_f = cos_b.astype(jnp.float32)
    sin_f = sin_b.astype(jnp.float32)
    spec_re = jnp.einsum('sfbd,bc->sfcd', twisted_re, cos_f) + jnp.einsum('sfbd,bc->sfcd', twisted_im, sin_f)
    spec_im = jnp.einsum('sfbd,bc->sfcd', twisted_im, cos_f) - jnp.einsum('sfbd,bc->sfcd', twisted_re, sin_f)
    return (spec_re.reshape(streams, frames, -1), spec_im.reshape(streams, frames, -1))

def reference(samples, filter_taps):
    streams = samples.shape[0]
    frames = samples.shape[1] // FFT_LEN
    signal = samples.astype(jnp.float32).reshape(streams, frames, FFT_LEN)
    extended = jnp.concatenate([jnp.zeros((streams, TAPS - 1, FFT_LEN), jnp.float32), signal], axis=1)
    weights = filter_taps.astype(jnp.float32)
    filtered = jnp.zeros((streams, frames, FFT_LEN), jnp.float32)
    for tap_index in range(TAPS):
        offset = TAPS - 1 - tap_index
        filtered = filtered + weights[tap_index] * extended[:, offset:offset + frames]
    filtered = filtered.astype(jnp.bfloat16)
    spec_re, spec_im = transform(filtered)
    spec_re = lax.optimization_barrier(spec_re.astype(jnp.bfloat16)).astype(jnp.float32)
    spec_im = lax.optimization_barrier(spec_im.astype(jnp.bfloat16)).astype(jnp.float32)
    power = lax.optimization_barrier(jnp.sum(spec_re * spec_re + spec_im * spec_im, axis=(1, 2)))
    gain = target_level / jnp.sqrt(power / (frames * CHANNELS) + epsilon)
    scaled = jnp.stack([spec_re, spec_im], axis=1) * gain[:, None, None, None]
    clipped = jnp.clip(scaled, -1.0, 1.0)
    return jnp.transpose(clipped, (0, 1, 3, 2)).astype(jnp.bfloat16)
```

```python
import functools

import jax
import jax.numpy as jnp
import numpy as np
from jax import lax
from jax.experimental import pallas as pl
from jax.experimental.pallas import tpu as pltpu
from jax.sharding import PartitionSpec as P

ROW_LEN = 128
LANES = 128
MESH = pl.DeviceIdType.MESH


def kernel_tables(row_len, col_len):
    fft_len = row_len * col_len
    a = np.arange(row_len)
    b = np.arange(col_len)
    c = np.arange(col_len // 2)
    pi2 = 2.0 * np.pi
    order = np.concatenate([a[0::2], a[1::2]])
    angle_a = (np.float32(pi2 / row_len) * (a[:, None] * order[None, :] % row_len).astype(np.float32)).astype(np.float64)
    stage_a = np.concatenate([np.cos(angle_a), -np.sin(angle_a)], axis=0)
    angle_t = (np.float32(pi2 / fft_len) * (a[:, None] * b[None, :] % fft_len).astype(np.float32)).astype(np.float64)
    cos_t = np.tile(np.cos(angle_t), (1, 2))
    sin_t = np.tile(np.sin(angle_t), (1, 2))
    angle_b = (np.float32(pi2 / col_len) * (c[:, None] * b[None, :] % col_len).astype(np.float32)).astype(np.float64)
    cos_b, sin_b = np.cos(angle_b), np.sin(angle_b)
    rows = 2 * len(c)
    stage_b = np.zeros((2 * rows, 4 * col_len))
    re_part = np.concatenate([cos_b, -sin_b], axis=0)
    im_part = np.concatenate([sin_b, cos_b], axis=0)
    for f in range(2):
        at = slice(f * rows, (f + 1) * rows)
        stage_b[at, f * col_len : (f + 1) * col_len] = re_part
        stage_b[at, (2 + f) * col_len : (3 + f) * col_len] = im_part
    return (
        jnp.asarray(stage_a, jnp.bfloat16),
        jnp.asarray(cos_t, jnp.float32),
        jnp.asarray(sin_t, jnp.float32),
        jnp.asarray(stage_b, jnp.bfloat16),
    )


def body(
    n, count, x_ref, taps_ref, ta_ref, ct_ref, st_ref, tb_ref, eye_ref, out_ref,
    xf, wf, ext, ybuf, gbuf, spec, recv, pbuf, pall, gain_buf,
    halo_send, halo_recv, spec_send, spec_recv, own_sem, pow_send, pow_recv, pow_own,
):
    me = lax.axis_index("tm")
    streams = x_ref.shape[0]
    taps, fft_len = taps_ref.shape
    hist = taps - 1
    frames = x_ref.shape[1] // fft_len
    rows = fft_len // LANES
    rc = gbuf.shape[0] // frames
    half_c = rc // 2
    ch = out_ref.shape[2]
    cb = ch // LANES

    barrier = pltpu.get_barrier_semaphore()

    @pl.loop(1, n)
    def _(o):
        pl.semaphore_signal(barrier, inc=1, device_id={"tm": lax.rem(me + o, n)}, device_id_type=MESH)

    unroll = 16

    @pl.loop(0, frames * rows // unroll)
    def _(i):
        for u in range(unroll):
            q = i * unroll + u
            v = x_ref[:, pl.ds(pl.multiple_of(q * LANES, LANES), LANES)].astype(jnp.float32)
            xf[pl.ds(q, streams, stride=frames * rows), :] = v

    @pl.loop(0, streams)
    def _(s):
        @pl.loop(0, frames)
        def _(f):
            at = pl.multiple_of((s * frames + f) * rows, rows)
            ext[s, hist + f] = xf[pl.ds(at, rows), :].astype(jnp.bfloat16)

    pl.semaphore_wait(barrier, n - 1)

    def halo_copy(s):
        return pltpu.make_async_remote_copy(
            src_ref=ext.at[s, pl.ds(frames, hist)],
            dst_ref=ext.at[s, pl.ds(0, hist)],
            send_sem=halo_send.at[s],
            recv_sem=halo_recv.at[s],
            device_id={"tm": lax.rem(me + 1, n)},
            device_id_type=MESH,
        )

    @pl.when(me < n - 1)
    def _():
        @pl.loop(0, streams)
        def _(s):
            halo_copy(s).start()

    @pl.when(me == 0)
    def _():
        @pl.loop(0, streams)
        def _(s):
            ext[s, pl.ds(0, hist)] = jnp.zeros((hist, rows, LANES), jnp.bfloat16)

    @pl.loop(0, rows)
    def _(r):
        w = taps_ref[:, pl.ds(pl.multiple_of(r * LANES, LANES), LANES)].astype(jnp.float32)
        wf[pl.ds(r, taps, stride=rows), :] = w

    low = lax.broadcasted_iota(jnp.int32, (16, LANES), 1) < LANES // 2

    @pl.loop(0, streams)
    def _(s):
        @pl.when(me > 0)
        def _():
            halo_copy(s).wait_recv()

        @pl.loop(0, rows // 16)
        def _(rb):
            r0 = pl.multiple_of(rb * 16, 16)
            acc = [None] * frames
            w = [wf[pl.ds(p * rows + r0, 16), :] for p in range(taps)]
            for i in range(hist + frames - 1, -1, -1):
                xi = ext[s, i, pl.ds(r0, 16), :].astype(jnp.float32)
                for f in range(frames):
                    p = f + hist - i
                    if 0 <= p < taps:
                        term = w[p] * xi
                        acc[f] = term if acc[f] is None else acc[f] + term
            for q in range(frames // 2):
                f0, f1 = acc[2 * q], acc[2 * q + 1]
                y0 = jnp.where(low, f0, pltpu.roll(f1, LANES // 2, 1))
                y1 = jnp.where(low, pltpu.roll(f0, LANES // 2, 1), f1)
                ybuf[q, pl.ds(r0, 16), :] = y0.astype(jnp.bfloat16)
                ybuf[q, pl.ds(rows + r0, 16), :] = y1.astype(jnp.bfloat16)

        @pl.loop(0, frames // 4)
        def _(g):
            y = jnp.concatenate([ybuf[2 * g], ybuf[2 * g + 1]], axis=1)
            first = jnp.dot(ta_ref[...], y, preferred_element_type=jnp.float32)
            for u in range(2):
                re = first[:ROW_LEN, u * LANES : (u + 1) * LANES]
                im = first[ROW_LEN:, u * LANES : (u + 1) * LANES]
                ct, st = ct_ref[...], st_ref[...]
                tw = jnp.concatenate(
                    [(re * ct + im * st).astype(jnp.bfloat16), (im * ct - re * st).astype(jnp.bfloat16)],
                    axis=1,
                )
                sp = lax.dot_general(
                    tb_ref[...], tw, (((1,), (1,)), ((), ())), preferred_element_type=jnp.float32
                )
                for f in range(2):
                    gbuf[pl.ds(4 * g + 2 * u + f, rc, stride=frames), :] = sp[f * rc : (f + 1) * rc]

        def pack(j, total):
            for ri in range(2):
                for cc in range(cb):
                    at = pl.multiple_of((ri * half_c + j * cb + cc) * frames, frames)
                    tile = gbuf[pl.ds(at, frames), :].astype(jnp.bfloat16)
                    spec[s, j, ri, :, pl.ds(cc * LANES, LANES)] = tile
                    wide = tile.astype(jnp.float32)
                    total = total + wide * wide
            return total

        total = lax.fori_loop(0, n, pack, jnp.zeros((frames, LANES), jnp.float32))
        pbuf[pl.ds(s, 1), :] = jnp.sum(total, axis=0, keepdims=True)

        @pl.loop(1, n)
        def _(o):
            peer = lax.rem(me + o, n)
            pltpu.make_async_remote_copy(
                src_ref=spec.at[s, peer],
                dst_ref=recv.at[s, :, pl.ds(me * frames, frames), :],
                send_sem=spec_send.at[s],
                recv_sem=spec_recv.at[s],
                device_id={"tm": peer},
                device_id_type=MESH,
            ).start()

        pltpu.make_async_copy(
            spec.at[s, me], recv.at[s, :, pl.ds(me * frames, frames), :], own_sem.at[s]
        ).start()

    @pl.loop(1, n)
    def _(o):
        peer = lax.rem(me + o, n)
        pltpu.make_async_remote_copy(
            src_ref=pbuf,
            dst_ref=pall.at[me],
            send_sem=pow_send,
            recv_sem=pow_recv,
            device_id={"tm": peer},
            device_id_type=MESH,
        ).start()

    mine = pltpu.make_async_copy(pbuf, pall.at[me], pow_own)
    mine.start()
    mine.wait()
    part = pall.at[pl.ds(0, n - 1)]
    pltpu.make_async_copy(part, part, pow_recv).wait()
    power = jnp.sum(jnp.sum(pall[...], axis=0), axis=1, keepdims=True)
    gain = 0.378 / jnp.sqrt(power / count + 1e-06)
    gain_buf[...] = jnp.broadcast_to(gain, gain_buf.shape)

    @pl.loop(0, streams)
    def _(s):
        others = spec.at[s, pl.ds(0, n - 1)]
        pltpu.make_async_copy(others, others, spec_recv.at[s]).wait()
        pltpu.make_async_copy(
            spec.at[s, me], recv.at[s, :, pl.ds(me * frames, frames), :], own_sem.at[s]
        ).wait()
        g = gain_buf[pl.ds(s, 1), :]
        for ri in range(2):
            flipped = lax.dot_general(
                eye_ref[...], recv[s, ri], (((1,), (1,)), ((), ())), preferred_element_type=jnp.float32
            )
            scaled = jnp.clip(flipped * g, -1.0, 1.0)
            out_ref[s, ri] = scaled.astype(jnp.bfloat16)

    @pl.loop(0, streams)
    def _(s):
        others = spec.at[s, pl.ds(0, n - 1)]
        pltpu.make_async_copy(others, others, spec_send.at[s]).wait()

    part = pall.at[pl.ds(0, n - 1)]
    pltpu.make_async_copy(part, part, pow_send).wait()

    @pl.when(me < n - 1)
    def _():
        @pl.loop(0, streams)
        def _(s):
            halo_copy(s).wait_send()


def on_device_kernel(samples, filter_taps):
    n = lax.axis_size("tm")
    streams = samples.shape[0]
    taps, fft_len = filter_taps.shape
    frames = samples.shape[1] // fft_len
    rows = fft_len // LANES
    col_len = fft_len // ROW_LEN
    channels = fft_len // 2
    ch = channels // n
    stage_a, cos_t, sin_t, stage_b = kernel_tables(ROW_LEN, col_len)
    eye = jnp.asarray(np.eye(ch), jnp.bfloat16)
    vmem = pl.BlockSpec(memory_space=pltpu.VMEM)
    dma = pltpu.SemaphoreType.DMA
    return pl.pallas_call(
        functools.partial(body, n, float(frames * n * channels)),
        out_shape=jax.ShapeDtypeStruct((streams, 2, ch, frames * n), jnp.bfloat16),
        in_specs=[vmem] * 7,
        out_specs=vmem,
        scratch_shapes=[
            pltpu.VMEM((streams * frames * rows, LANES), jnp.float32),
            pltpu.VMEM((taps * rows, LANES), jnp.float32),
            pltpu.VMEM((streams, frames + taps - 1, rows, LANES), jnp.bfloat16),
            pltpu.VMEM((frames // 2, 2 * rows, LANES), jnp.bfloat16),
            pltpu.VMEM((col_len * frames, LANES), jnp.float32),
            pltpu.VMEM((streams, n, 2, frames, ch), jnp.bfloat16),
            pltpu.VMEM((streams, 2, frames * n, ch), jnp.bfloat16),
            pltpu.VMEM((streams, LANES), jnp.float32),
            pltpu.VMEM((n, streams, LANES), jnp.float32),
            pltpu.VMEM((streams, frames * n), jnp.float32),
            dma((streams,)), dma((streams,)), dma((streams,)), dma((streams,)), dma((streams,)),
            dma, dma, dma,
        ],
        compiler_params=pltpu.CompilerParams(
            collective_id=0, has_side_effects=True, vmem_limit_bytes=60 * 1024 * 1024
        ),
    )(samples, filter_taps, stage_a, cos_t, sin_t, stage_b, eye)


target_level = 0.378
epsilon = 1e-06


def shifted(value, axis, by):
    size = lax.axis_size(axis)
    pairs = [(i, i + by) for i in range(size) if 0 <= i + by < size]
    return lax.ppermute(value, axis, pairs)


def tables(row_len, col_len):
    fft_len = row_len * col_len
    rows_a = jnp.arange(row_len, dtype=jnp.int32)
    cols_b = jnp.arange(col_len, dtype=jnp.int32)
    half_c = jnp.arange(col_len // 2, dtype=jnp.int32)
    angle_a = (
        2.0 * jnp.pi / row_len * (rows_a[:, None] * rows_a[None, :] % row_len).astype(jnp.float32)
    )
    angle_t = (
        2.0 * jnp.pi / fft_len * (cols_b[:, None] * rows_a[None, :] % fft_len).astype(jnp.float32)
    )
    angle_b = (
        2.0 * jnp.pi / col_len * (cols_b[:, None] * half_c[None, :] % col_len).astype(jnp.float32)
    )
    return (
        jnp.cos(angle_a).astype(jnp.bfloat16),
        jnp.sin(angle_a).astype(jnp.bfloat16),
        jnp.cos(angle_t),
        jnp.sin(angle_t),
        jnp.cos(angle_b).astype(jnp.bfloat16),
        jnp.sin(angle_b).astype(jnp.bfloat16),
    )


def transform(filtered):
    streams, frames, fft_len = filtered.shape
    col_len = fft_len // ROW_LEN
    cos_a, sin_a, cos_t, sin_t, cos_b, sin_b = tables(ROW_LEN, col_len)
    blocks = filtered.reshape(streams, frames, ROW_LEN, col_len)
    first_re = jnp.einsum("sfab,ad->sfbd", blocks, cos_a, preferred_element_type=jnp.float32)
    first_im = -jnp.einsum("sfab,ad->sfbd", blocks, sin_a, preferred_element_type=jnp.float32)
    twisted_re = (first_re * cos_t + first_im * sin_t).astype(jnp.bfloat16)
    twisted_im = (first_im * cos_t - first_re * sin_t).astype(jnp.bfloat16)
    spec_re = jnp.einsum(
        "sfbd,bc->scdf", twisted_re, cos_b, preferred_element_type=jnp.float32
    ) + jnp.einsum("sfbd,bc->scdf", twisted_im, sin_b, preferred_element_type=jnp.float32)
    spec_im = jnp.einsum(
        "sfbd,bc->scdf", twisted_im, cos_b, preferred_element_type=jnp.float32
    ) - jnp.einsum("sfbd,bc->scdf", twisted_re, sin_b, preferred_element_type=jnp.float32)
    return (spec_re.reshape(streams, -1, frames), spec_im.reshape(streams, -1, frames))


def on_device(samples, filter_taps):
    streams = samples.shape[0]
    tap_count, fft_len = filter_taps.shape
    frames = samples.shape[1] // fft_len
    signal = samples.reshape(streams, frames, fft_len)
    history = shifted(signal[:, frames - (tap_count - 1) :, :], "tm", 1)
    extended = jnp.concatenate([history, signal], axis=1)
    weights = filter_taps.astype(jnp.float32)
    filtered = jnp.zeros((streams, frames, fft_len), jnp.float32)
    for tap_index in range(tap_count):
        offset = tap_count - 1 - tap_index
        filtered = filtered + weights[tap_index] * extended[:, offset : offset + frames].astype(
            jnp.float32
        )
    filtered = filtered.astype(jnp.bfloat16)
    spec_re, spec_im = transform(filtered)
    real_part = spec_re.astype(jnp.bfloat16)
    imag_part = spec_im.astype(jnp.bfloat16)
    real_wide = real_part.astype(jnp.float32)
    imag_wide = imag_part.astype(jnp.float32)
    local_power = jnp.sum(real_wide * real_wide + imag_wide * imag_wide, axis=(1, 2))
    total_power = lax.psum(local_power, "tm")
    count = frames * lax.axis_size("tm") * spec_re.shape[1]
    gain = target_level / jnp.sqrt(total_power / count + epsilon)
    scaled = jnp.stack(
        [
            jnp.clip(real_wide * gain[:, None, None], -1.0, 1.0),
            jnp.clip(imag_wide * gain[:, None, None], -1.0, 1.0),
        ],
        axis=1,
    ).astype(jnp.bfloat16)
    result = lax.all_to_all(scaled, "tm", split_axis=2, concat_axis=3, tiled=True)
    return result


def solution(mesh):
    tm = mesh.shape["tm"]

    def on_shard(samples, filter_taps):
        fft_len = filter_taps.shape[1]
        frames = samples.shape[1] // fft_len
        whole_tiles = (fft_len // 2) % (tm * LANES) == 0 and (frames * tm) % LANES == 0
        if whole_tiles and frames % 16 == 0 and fft_len == LANES * (LANES // 2):
            return on_device_kernel(samples, filter_taps)
        return on_device(samples, filter_taps)

    return jax.shard_map(
        on_shard,
        mesh=mesh,
        in_specs=(P("grp", "tm"), P()),
        out_specs=P("grp", None, "tm", None),
        check_vma=False,
    )
```

```python
import functools

import jax
import jax.numpy as jnp
import numpy as np
from jax import lax
from jax.experimental import pallas as pl
from jax.experimental.pallas import tpu as pltpu
from jax.sharding import PartitionSpec as P

ROW_LEN = 128
LANES = 128
TURN = 4
RELAY = -3
VMEM_MIB = 60
X_PIECES = 4
MESH = pl.DeviceIdType.MESH


def kernel_tables(row_len, col_len):
    fft_len = row_len * col_len
    a = np.arange(row_len)
    b = np.arange(col_len)
    c = np.arange(col_len // 2)
    pi2 = 2.0 * np.pi
    order = np.concatenate([a[0::2], a[1::2]])
    angle_a = (np.float32(pi2 / row_len) * (a[:, None] * order[None, :] % row_len).astype(np.float32)).astype(np.float64)
    stage_a = np.concatenate([np.cos(angle_a), -np.sin(angle_a)], axis=0)
    angle_t = (np.float32(pi2 / fft_len) * (a[:, None] * b[None, :] % fft_len).astype(np.float32)).astype(np.float64)
    cos_t = np.tile(np.cos(angle_t), (1, 2))
    sin_t = np.tile(np.sin(angle_t), (1, 2))
    angle_b = (np.float32(pi2 / col_len) * (c[:, None] * b[None, :] % col_len).astype(np.float32)).astype(np.float64)
    cos_b, sin_b = np.cos(angle_b), np.sin(angle_b)
    rows = 2 * len(c)
    stage_b = np.zeros((2 * rows, 4 * col_len))
    re_part = np.concatenate([cos_b, -sin_b], axis=0)
    im_part = np.concatenate([sin_b, cos_b], axis=0)
    for f in range(2):
        at = slice(f * rows, (f + 1) * rows)
        stage_b[at, f * col_len : (f + 1) * col_len] = re_part
        stage_b[at, (2 + f) * col_len : (3 + f) * col_len] = im_part
    return (
        jnp.asarray(stage_a, jnp.bfloat16),
        jnp.asarray(cos_t, jnp.float32),
        jnp.asarray(sin_t, jnp.float32),
        jnp.asarray(stage_b, jnp.bfloat16),
    )


def body(
    n, count, x_hbm, taps_hbm, ta_hbm, ct_hbm, st_hbm, tb_hbm, eye_hbm, out_hbm,
    x_ref, taps_ref, ta_ref, ct_ref, st_ref, tb_ref, eye_ref, out_ref, relay, xf, wf, ext, ybuf, gbuf, spec, recv, pbuf, pall, gain_buf,
    halo_send, halo_recv, spec_send, spec_recv, own_sem, pow_send, pow_recv, pow_own,
    relay_send, relay_recv, x_sem, const_sem, out_sem,
):
    me = lax.axis_index("tm")
    streams = x_ref.shape[0]
    taps, fft_len = taps_ref.shape
    hist = taps - 1
    frames = x_ref.shape[1] // fft_len
    rows = fft_len // LANES
    rc = gbuf.shape[0] // frames
    half_c = rc // 2
    ch = out_ref.shape[2]
    cb = ch // LANES

    barrier = pltpu.get_barrier_semaphore()

    @pl.loop(1, n)
    def _(o):
        pl.semaphore_signal(barrier, inc=1, device_id={"tm": lax.rem(me + o, n)}, device_id_type=MESH)

    piece = x_ref.shape[1] // X_PIECES

    def x_copy(i):
        at = pl.ds(pl.multiple_of(i * piece, piece), piece)
        return pltpu.make_async_copy(x_hbm.at[:, at], x_ref.at[:, at], x_sem.at[i])

    @pl.loop(0, X_PIECES)
    def _(i):
        x_copy(i).start()

    tables = [
        (taps_hbm, taps_ref), (ta_hbm, ta_ref), (ct_hbm, ct_ref),
        (st_hbm, st_ref), (tb_hbm, tb_ref), (eye_hbm, eye_ref),
    ]
    fetches = [pltpu.make_async_copy(a, b, const_sem.at[i]) for i, (a, b) in enumerate(tables)]
    for fetch in fetches:
        fetch.start()

    unroll = 16

    steps = frames * rows // unroll // X_PIECES

    @pl.loop(0, X_PIECES)
    def _(c):
        x_copy(c).wait()

        @pl.loop(0, steps)
        def _(i):
            for u in range(unroll):
                q = (c * steps + i) * unroll + u
                v = x_ref[:, pl.ds(pl.multiple_of(q * LANES, LANES), LANES)].astype(jnp.float32)
                xf[pl.ds(q, streams, stride=frames * rows), :] = v

    half_s = streams // 2
    turns = jnp.logical_and(lax.rem(me, TURN) == TURN - 1, me < n - 1)
    relayed = jnp.logical_and(turns, jnp.logical_and(me + RELAY >= 0, me + RELAY < n))
    source = me - RELAY
    relays = jnp.logical_and(
        jnp.logical_and(source >= 0, source < n - 1), lax.rem(source + n, TURN) == TURN - 1
    )
    direct = jnp.logical_and(me < n - 1, jnp.logical_not(relayed))

    def halo_copy(s):
        return pltpu.make_async_remote_copy(
            src_ref=ext.at[s, pl.ds(frames, hist)],
            dst_ref=ext.at[s, pl.ds(0, hist)],
            send_sem=halo_send.at[s],
            recv_sem=halo_recv.at[s],
            device_id={"tm": lax.rem(me + 1, n)},
            device_id_type=MESH,
        )

    def to_relay(s):
        return pltpu.make_async_remote_copy(
            src_ref=ext.at[s, pl.ds(frames, hist)],
            dst_ref=relay.at[s - half_s],
            send_sem=halo_send.at[s],
            recv_sem=relay_recv.at[s - half_s],
            device_id={"tm": lax.rem(me + RELAY + n, n)},
            device_id_type=MESH,
        )

    def from_relay(s):
        return pltpu.make_async_remote_copy(
            src_ref=relay.at[s - half_s],
            dst_ref=ext.at[s, pl.ds(0, hist)],
            send_sem=relay_send.at[s - half_s],
            recv_sem=halo_recv.at[s],
            device_id={"tm": lax.rem(source + 1 + n, n)},
            device_id_type=MESH,
        )

    def convert(s):
        @pl.loop(0, frames)
        def _(f):
            at = pl.multiple_of((s * frames + f) * rows, rows)
            ext[s, hist + f] = xf[pl.ds(at, rows), :].astype(jnp.bfloat16)

    pl.semaphore_wait(barrier, n - 1)

    @pl.loop(0, half_s)
    def _(s):
        convert(s)
        convert(s + half_s)

        @pl.when(me < n - 1)
        def _():
            halo_copy(s).start()

        @pl.when(direct)
        def _():
            halo_copy(s + half_s).start()

        @pl.when(relayed)
        def _():
            to_relay(s + half_s).start()

    @pl.when(me == 0)
    def _():
        @pl.loop(0, streams)
        def _(s):
            ext[s, pl.ds(0, hist)] = jnp.zeros((hist, rows, LANES), jnp.bfloat16)

    for fetch in fetches:
        fetch.wait()

    @pl.loop(0, rows)
    def _(r):
        w = taps_ref[:, pl.ds(pl.multiple_of(r * LANES, LANES), LANES)].astype(jnp.float32)
        wf[pl.ds(r, taps, stride=rows), :] = w

    low = lax.broadcasted_iota(jnp.int32, (16, LANES), 1) < LANES // 2

    @pl.loop(0, streams)
    def _(s):
        @pl.when(me > 0)
        def _():
            halo_copy(s).wait_recv()

        @pl.when(jnp.logical_and(relays, s < half_s))
        def _():
            to_relay(s + half_s).wait_recv()
            from_relay(s + half_s).start()

        @pl.loop(0, rows // 16)
        def _(rb):
            r0 = pl.multiple_of(rb * 16, 16)
            acc = [None] * frames
            w = [wf[pl.ds(p * rows + r0, 16), :] for p in range(taps)]
            for i in range(hist + frames - 1, -1, -1):
                xi = ext[s, i, pl.ds(r0, 16), :].astype(jnp.float32)
                for f in range(frames):
                    p = f + hist - i
                    if 0 <= p < taps:
                        term = w[p] * xi
                        acc[f] = term if acc[f] is None else acc[f] + term
            for q in range(frames // 2):
                f0, f1 = acc[2 * q], acc[2 * q + 1]
                y0 = jnp.where(low, f0, pltpu.roll(f1, LANES // 2, 1))
                y1 = jnp.where(low, pltpu.roll(f0, LANES // 2, 1), f1)
                ybuf[q, pl.ds(r0, 16), :] = y0.astype(jnp.bfloat16)
                ybuf[q, pl.ds(rows + r0, 16), :] = y1.astype(jnp.bfloat16)

        @pl.loop(0, frames // 4)
        def _(g):
            y = jnp.concatenate([ybuf[2 * g], ybuf[2 * g + 1]], axis=1)
            first = jnp.dot(ta_ref[...], y, preferred_element_type=jnp.float32)
            for u in range(2):
                re = first[:ROW_LEN, u * LANES : (u + 1) * LANES]
                im = first[ROW_LEN:, u * LANES : (u + 1) * LANES]
                ct, st = ct_ref[...], st_ref[...]
                tw = jnp.concatenate(
                    [(re * ct + im * st).astype(jnp.bfloat16), (im * ct - re * st).astype(jnp.bfloat16)],
                    axis=1,
                )
                sp = lax.dot_general(
                    tb_ref[...], tw, (((1,), (1,)), ((), ())), preferred_element_type=jnp.float32
                )
                for f in range(2):
                    gbuf[pl.ds(4 * g + 2 * u + f, rc, stride=frames), :] = sp[f * rc : (f + 1) * rc]

        def pack(j, total):
            for ri in range(2):
                for cc in range(cb):
                    at = pl.multiple_of((ri * half_c + j * cb + cc) * frames, frames)
                    tile = gbuf[pl.ds(at, frames), :].astype(jnp.bfloat16)
                    spec[s, j, ri, :, pl.ds(cc * LANES, LANES)] = tile
                    wide = tile.astype(jnp.float32)
                    total = total + wide * wide
            return total

        total = lax.fori_loop(0, n, pack, jnp.zeros((frames, LANES), jnp.float32))
        pbuf[pl.ds(s, 1), :] = jnp.sum(total, axis=0, keepdims=True)

        def send(peer):
            pltpu.make_async_remote_copy(
                src_ref=spec.at[s, peer],
                dst_ref=recv.at[s, :, pl.ds(me * frames, frames), :],
                send_sem=spec_send.at[s],
                recv_sem=spec_recv.at[s],
                device_id={"tm": peer},
                device_id_type=MESH,
            ).start()

        @pl.loop(0, n // 2)
        def _(o):
            send((1 - me // (n // 2)) * (n // 2) + lax.rem(me + o, n // 2))

        @pl.loop(1, n // 2)
        def _(o):
            send(me // (n // 2) * (n // 2) + lax.rem(me + o, n // 2))

        pltpu.make_async_copy(
            spec.at[s, me], recv.at[s, :, pl.ds(me * frames, frames), :], own_sem.at[s]
        ).start()

    @pl.loop(1, n)
    def _(o):
        peer = lax.rem(me + o, n)
        pltpu.make_async_remote_copy(
            src_ref=pbuf,
            dst_ref=pall.at[me],
            send_sem=pow_send,
            recv_sem=pow_recv,
            device_id={"tm": peer},
            device_id_type=MESH,
        ).start()

    mine = pltpu.make_async_copy(pbuf, pall.at[me], pow_own)
    mine.start()
    mine.wait()
    part = pall.at[pl.ds(0, n - 1)]
    pltpu.make_async_copy(part, part, pow_recv).wait()
    power = jnp.sum(jnp.sum(pall[...], axis=0), axis=1, keepdims=True)
    gain = 0.378 / jnp.sqrt(power / count + 1e-06)
    gain_buf[...] = jnp.broadcast_to(gain, gain_buf.shape)

    @pl.loop(0, streams)
    def _(s):
        others = spec.at[s, pl.ds(0, n - 1)]
        pltpu.make_async_copy(others, others, spec_recv.at[s]).wait()
        pltpu.make_async_copy(
            spec.at[s, me], recv.at[s, :, pl.ds(me * frames, frames), :], own_sem.at[s]
        ).wait()
        g = gain_buf[pl.ds(s, 1), :]
        for ri in range(2):
            flipped = lax.dot_general(
                eye_ref[...], recv[s, ri], (((1,), (1,)), ((), ())), preferred_element_type=jnp.float32
            )
            scaled = jnp.clip(flipped * g, -1.0, 1.0)
            out_ref[s, ri] = scaled.astype(jnp.bfloat16)
        pltpu.make_async_copy(out_ref.at[s], out_hbm.at[s], out_sem.at[s]).start()

    @pl.loop(0, streams)
    def _(s):
        others = spec.at[s, pl.ds(0, n - 1)]
        pltpu.make_async_copy(others, others, spec_send.at[s]).wait()

    part = pall.at[pl.ds(0, n - 1)]
    pltpu.make_async_copy(part, part, pow_send).wait()

    @pl.when(me < n - 1)
    def _():
        @pl.loop(0, streams)
        def _(s):
            halo_copy(s).wait_send()

    @pl.when(relays)
    def _():
        @pl.loop(0, half_s)
        def _(s):
            from_relay(s + half_s).wait_send()

    @pl.loop(0, streams)
    def _(s):
        pltpu.make_async_copy(out_ref.at[s], out_hbm.at[s], out_sem.at[s]).wait()


def on_device_kernel(samples, filter_taps):
    n = lax.axis_size("tm")
    streams = samples.shape[0]
    taps, fft_len = filter_taps.shape
    frames = samples.shape[1] // fft_len
    rows = fft_len // LANES
    col_len = fft_len // ROW_LEN
    channels = fft_len // 2
    ch = channels // n
    stage_a, cos_t, sin_t, stage_b = kernel_tables(ROW_LEN, col_len)
    eye = jnp.asarray(np.eye(ch), jnp.bfloat16)
    hbm = pl.BlockSpec(memory_space=pl.ANY)
    dma = pltpu.SemaphoreType.DMA
    return pl.pallas_call(
        functools.partial(body, n, float(frames * n * channels)),
        out_shape=jax.ShapeDtypeStruct((streams, 2, ch, frames * n), jnp.bfloat16),
        in_specs=[hbm] * 7,
        out_specs=hbm,
        scratch_shapes=[
            pltpu.VMEM(samples.shape, samples.dtype),
            pltpu.VMEM(filter_taps.shape, filter_taps.dtype),
            *[pltpu.VMEM(t.shape, t.dtype) for t in (stage_a, cos_t, sin_t, stage_b, eye)],
            pltpu.VMEM((streams, 2, ch, frames * n), jnp.bfloat16),
            pltpu.VMEM((streams // 2, taps - 1, rows, LANES), jnp.bfloat16),
            pltpu.VMEM((streams * frames * rows, LANES), jnp.float32),
            pltpu.VMEM((taps * rows, LANES), jnp.float32),
            pltpu.VMEM((streams, frames + taps - 1, rows, LANES), jnp.bfloat16),
            pltpu.VMEM((frames // 2, 2 * rows, LANES), jnp.bfloat16),
            pltpu.VMEM((col_len * frames, LANES), jnp.float32),
            pltpu.VMEM((streams, n, 2, frames, ch), jnp.bfloat16),
            pltpu.VMEM((streams, 2, frames * n, ch), jnp.bfloat16),
            pltpu.VMEM((streams, LANES), jnp.float32),
            pltpu.VMEM((n, streams, LANES), jnp.float32),
            pltpu.VMEM((streams, frames * n), jnp.float32),
            dma((streams,)), dma((streams,)), dma((streams,)), dma((streams,)), dma((streams,)),
            dma, dma, dma,
            dma((streams // 2,)), dma((streams // 2,)), dma((X_PIECES,)), dma((6,)), dma((streams,)),
        ],
        compiler_params=pltpu.CompilerParams(
            collective_id=0, has_side_effects=True, vmem_limit_bytes=VMEM_MIB * 1024 * 1024
        ),
    )(samples, filter_taps, stage_a, cos_t, sin_t, stage_b, eye)


target_level = 0.378
epsilon = 1e-06


def shifted(value, axis, by):
    size = lax.axis_size(axis)
    pairs = [(i, i + by) for i in range(size) if 0 <= i + by < size]
    return lax.ppermute(value, axis, pairs)


def tables(row_len, col_len):
    fft_len = row_len * col_len
    rows_a = jnp.arange(row_len, dtype=jnp.int32)
    cols_b = jnp.arange(col_len, dtype=jnp.int32)
    half_c = jnp.arange(col_len // 2, dtype=jnp.int32)
    angle_a = (
        2.0 * jnp.pi / row_len * (rows_a[:, None] * rows_a[None, :] % row_len).astype(jnp.float32)
    )
    angle_t = (
        2.0 * jnp.pi / fft_len * (cols_b[:, None] * rows_a[None, :] % fft_len).astype(jnp.float32)
    )
    angle_b = (
        2.0 * jnp.pi / col_len * (cols_b[:, None] * half_c[None, :] % col_len).astype(jnp.float32)
    )
    return (
        jnp.cos(angle_a).astype(jnp.bfloat16),
        jnp.sin(angle_a).astype(jnp.bfloat16),
        jnp.cos(angle_t),
        jnp.sin(angle_t),
        jnp.cos(angle_b).astype(jnp.bfloat16),
        jnp.sin(angle_b).astype(jnp.bfloat16),
    )


def transform(filtered):
    streams, frames, fft_len = filtered.shape
    col_len = fft_len // ROW_LEN
    cos_a, sin_a, cos_t, sin_t, cos_b, sin_b = tables(ROW_LEN, col_len)
    blocks = filtered.reshape(streams, frames, ROW_LEN, col_len)
    first_re = jnp.einsum("sfab,ad->sfbd", blocks, cos_a, preferred_element_type=jnp.float32)
    first_im = -jnp.einsum("sfab,ad->sfbd", blocks, sin_a, preferred_element_type=jnp.float32)
    twisted_re = (first_re * cos_t + first_im * sin_t).astype(jnp.bfloat16)
    twisted_im = (first_im * cos_t - first_re * sin_t).astype(jnp.bfloat16)
    spec_re = jnp.einsum(
        "sfbd,bc->scdf", twisted_re, cos_b, preferred_element_type=jnp.float32
    ) + jnp.einsum("sfbd,bc->scdf", twisted_im, sin_b, preferred_element_type=jnp.float32)
    spec_im = jnp.einsum(
        "sfbd,bc->scdf", twisted_im, cos_b, preferred_element_type=jnp.float32
    ) - jnp.einsum("sfbd,bc->scdf", twisted_re, sin_b, preferred_element_type=jnp.float32)
    return (spec_re.reshape(streams, -1, frames), spec_im.reshape(streams, -1, frames))


def on_device(samples, filter_taps):
    streams = samples.shape[0]
    tap_count, fft_len = filter_taps.shape
    frames = samples.shape[1] // fft_len
    signal = samples.reshape(streams, frames, fft_len)
    history = shifted(signal[:, frames - (tap_count - 1) :, :], "tm", 1)
    extended = jnp.concatenate([history, signal], axis=1)
    weights = filter_taps.astype(jnp.float32)
    filtered = jnp.zeros((streams, frames, fft_len), jnp.float32)
    for tap_index in range(tap_count):
        offset = tap_count - 1 - tap_index
        filtered = filtered + weights[tap_index] * extended[:, offset : offset + frames].astype(
            jnp.float32
        )
    filtered = filtered.astype(jnp.bfloat16)
    spec_re, spec_im = transform(filtered)
    real_part = spec_re.astype(jnp.bfloat16)
    imag_part = spec_im.astype(jnp.bfloat16)
    real_wide = real_part.astype(jnp.float32)
    imag_wide = imag_part.astype(jnp.float32)
    local_power = jnp.sum(real_wide * real_wide + imag_wide * imag_wide, axis=(1, 2))
    total_power = lax.psum(local_power, "tm")
    count = frames * lax.axis_size("tm") * spec_re.shape[1]
    gain = target_level / jnp.sqrt(total_power / count + epsilon)
    scaled = jnp.stack(
        [
            jnp.clip(real_wide * gain[:, None, None], -1.0, 1.0),
            jnp.clip(imag_wide * gain[:, None, None], -1.0, 1.0),
        ],
        axis=1,
    ).astype(jnp.bfloat16)
    result = lax.all_to_all(scaled, "tm", split_axis=2, concat_axis=3, tiled=True)
    return result


def solution(mesh):
    tm = mesh.shape["tm"]

    def on_shard(samples, filter_taps):
        fft_len = filter_taps.shape[1]
        frames = samples.shape[1] // fft_len
        whole_tiles = (fft_len // 2) % (tm * LANES) == 0 and (frames * tm) % LANES == 0
        if whole_tiles and frames % 16 == 0 and fft_len == LANES * (LANES // 2) and tm % 2 == 0:
            return on_device_kernel(samples, filter_taps)
        return on_device(samples, filter_taps)

    return jax.shard_map(
        on_shard,
        mesh=mesh,
        in_specs=(P("grp", "tm"), P()),
        out_specs=P("grp", None, "tm", None),
        check_vma=False,
    )
```

```python
import functools

import jax
import jax.numpy as jnp
import numpy as np
from jax import lax
from jax.experimental import pallas as pl
from jax.experimental.pallas import tpu as pltpu
from jax.sharding import PartitionSpec as P

ROW_LEN = 128
LANES = 128
TURN = 4
RELAY = -3
VMEM_MIB = 60
X_PIECES = 4
MESH = pl.DeviceIdType.MESH


def kernel_tables(row_len, col_len):
    fft_len = row_len * col_len
    a = np.arange(row_len)
    b = np.arange(col_len)
    c = np.arange(col_len // 2)
    pi2 = 2.0 * np.pi
    order = np.concatenate([a[0::2], a[1::2]])
    angle_a = (np.float32(pi2 / row_len) * (a[:, None] * order[None, :] % row_len).astype(np.float32)).astype(np.float64)
    stage_a = np.concatenate([np.cos(angle_a), -np.sin(angle_a)], axis=0)
    angle_t = (np.float32(pi2 / fft_len) * (a[:, None] * b[None, :] % fft_len).astype(np.float32)).astype(np.float64)
    cos_t = np.tile(np.cos(angle_t), (1, 2))
    sin_t = np.tile(np.sin(angle_t), (1, 2))
    angle_b = (np.float32(pi2 / col_len) * (c[:, None] * b[None, :] % col_len).astype(np.float32)).astype(np.float64)
    cos_b, sin_b = np.cos(angle_b), np.sin(angle_b)
    rows = 2 * len(c)
    stage_b = np.zeros((2 * rows, 4 * col_len))
    re_part = np.concatenate([cos_b, -sin_b], axis=0)
    im_part = np.concatenate([sin_b, cos_b], axis=0)
    for f in range(2):
        at = slice(f * rows, (f + 1) * rows)
        stage_b[at, f * col_len : (f + 1) * col_len] = re_part
        stage_b[at, (2 + f) * col_len : (3 + f) * col_len] = im_part
    return (
        jnp.asarray(stage_a, jnp.bfloat16),
        jnp.asarray(cos_t, jnp.float32),
        jnp.asarray(sin_t, jnp.float32),
        jnp.asarray(stage_b, jnp.bfloat16),
    )


def body(
    n, count, x_hbm, taps_hbm, ta_hbm, ct_hbm, st_hbm, tb_hbm, eye_hbm, out_hbm,
    x_ref, taps_ref, ta_ref, ct_ref, st_ref, tb_ref, eye_ref, out_ref, relay, xf, wf, ext, ybuf, gbuf, spec, recv, pall,
    halo_send, halo_recv, spec_send, spec_recv, own_sem, pow_send, pow_recv,
    relay_send, relay_recv, x_sem, const_sem, out_sem,
):
    me = lax.axis_index("tm")
    streams = x_ref.shape[0]
    taps, fft_len = taps_ref.shape
    hist = taps - 1
    frames = x_ref.shape[1] // fft_len
    rows = fft_len // LANES
    rc = gbuf.shape[0] // frames
    half_c = rc // 2
    ch = out_ref.shape[2]
    cb = ch // LANES

    barrier = pltpu.get_barrier_semaphore()

    @pl.loop(1, n)
    def _(o):
        pl.semaphore_signal(barrier, inc=1, device_id={"tm": lax.rem(me + o, n)}, device_id_type=MESH)

    piece = x_ref.shape[1] // X_PIECES

    def x_copy(i):
        at = pl.ds(pl.multiple_of(i * piece, piece), piece)
        return pltpu.make_async_copy(x_hbm.at[:, at], x_ref.at[:, at], x_sem.at[i])

    @pl.loop(0, X_PIECES)
    def _(i):
        x_copy(i).start()

    tables = [
        (taps_hbm, taps_ref), (ta_hbm, ta_ref), (ct_hbm, ct_ref),
        (st_hbm, st_ref), (tb_hbm, tb_ref), (eye_hbm, eye_ref),
    ]
    fetches = [pltpu.make_async_copy(a, b, const_sem.at[i]) for i, (a, b) in enumerate(tables)]
    for fetch in fetches:
        fetch.start()

    unroll = 16

    steps = frames * rows // unroll // X_PIECES

    @pl.loop(0, X_PIECES)
    def _(c):
        x_copy(c).wait()

        @pl.loop(0, steps)
        def _(i):
            for u in range(unroll):
                q = (c * steps + i) * unroll + u
                v = x_ref[:, pl.ds(pl.multiple_of(q * LANES, LANES), LANES)].astype(jnp.float32)
                xf[pl.ds(q, streams, stride=frames * rows), :] = v

    half_s = streams // 2
    turns = jnp.logical_and(lax.rem(me, TURN) == TURN - 1, me < n - 1)
    relayed = jnp.logical_and(turns, jnp.logical_and(me + RELAY >= 0, me + RELAY < n))
    source = me - RELAY
    relays = jnp.logical_and(
        jnp.logical_and(source >= 0, source < n - 1), lax.rem(source + n, TURN) == TURN - 1
    )
    direct = jnp.logical_and(me < n - 1, jnp.logical_not(relayed))

    def halo_copy(s):
        return pltpu.make_async_remote_copy(
            src_ref=ext.at[s, pl.ds(frames, hist)],
            dst_ref=ext.at[s, pl.ds(0, hist)],
            send_sem=halo_send.at[s],
            recv_sem=halo_recv.at[s],
            device_id={"tm": lax.rem(me + 1, n)},
            device_id_type=MESH,
        )

    def to_relay(s):
        return pltpu.make_async_remote_copy(
            src_ref=ext.at[s, pl.ds(frames, hist)],
            dst_ref=relay.at[s - half_s],
            send_sem=halo_send.at[s],
            recv_sem=relay_recv.at[s - half_s],
            device_id={"tm": lax.rem(me + RELAY + n, n)},
            device_id_type=MESH,
        )

    def from_relay(s):
        return pltpu.make_async_remote_copy(
            src_ref=relay.at[s - half_s],
            dst_ref=ext.at[s, pl.ds(0, hist)],
            send_sem=relay_send.at[s - half_s],
            recv_sem=halo_recv.at[s],
            device_id={"tm": lax.rem(source + 1 + n, n)},
            device_id_type=MESH,
        )

    def convert(s):
        @pl.loop(0, frames)
        def _(f):
            at = pl.multiple_of((s * frames + f) * rows, rows)
            ext[s, hist + f] = xf[pl.ds(at, rows), :].astype(jnp.bfloat16)

    pl.semaphore_wait(barrier, n - 1)

    @pl.loop(0, half_s)
    def _(s):
        convert(s)
        convert(s + half_s)

        @pl.when(me < n - 1)
        def _():
            halo_copy(s).start()

        @pl.when(direct)
        def _():
            halo_copy(s + half_s).start()

        @pl.when(relayed)
        def _():
            to_relay(s + half_s).start()

    @pl.when(me == 0)
    def _():
        @pl.loop(0, streams)
        def _(s):
            ext[s, pl.ds(0, hist)] = jnp.zeros((hist, rows, LANES), jnp.bfloat16)

    for fetch in fetches:
        fetch.wait()

    @pl.loop(0, rows)
    def _(r):
        w = taps_ref[:, pl.ds(pl.multiple_of(r * LANES, LANES), LANES)].astype(jnp.float32)
        wf[pl.ds(r, taps, stride=rows), :] = w

    low = lax.broadcasted_iota(jnp.int32, (16, LANES), 1) < LANES // 2

    @pl.loop(0, streams)
    def _(s):
        @pl.when(me > 0)
        def _():
            halo_copy(s).wait_recv()

        @pl.when(jnp.logical_and(relays, s < half_s))
        def _():
            to_relay(s + half_s).wait_recv()
            from_relay(s + half_s).start()

        @pl.loop(0, rows // 16)
        def _(rb):
            r0 = pl.multiple_of(rb * 16, 16)
            acc = [None] * frames
            w = [wf[pl.ds(p * rows + r0, 16), :] for p in range(taps)]
            for i in range(hist + frames - 1, -1, -1):
                xi = ext[s, i, pl.ds(r0, 16), :].astype(jnp.float32)
                for f in range(frames):
                    p = f + hist - i
                    if 0 <= p < taps:
                        term = w[p] * xi
                        acc[f] = term if acc[f] is None else acc[f] + term
            for q in range(frames // 2):
                f0, f1 = acc[2 * q], acc[2 * q + 1]
                y0 = jnp.where(low, f0, pltpu.roll(f1, LANES // 2, 1))
                y1 = jnp.where(low, pltpu.roll(f0, LANES // 2, 1), f1)
                ybuf[q, pl.ds(r0, 16), :] = y0.astype(jnp.bfloat16)
                ybuf[q, pl.ds(rows + r0, 16), :] = y1.astype(jnp.bfloat16)

        @pl.loop(0, frames // 4)
        def _(g):
            y = jnp.concatenate([ybuf[2 * g], ybuf[2 * g + 1]], axis=1)
            first = jnp.dot(ta_ref[...], y, preferred_element_type=jnp.float32)
            for u in range(2):
                re = first[:ROW_LEN, u * LANES : (u + 1) * LANES]
                im = first[ROW_LEN:, u * LANES : (u + 1) * LANES]
                ct, st = ct_ref[...], st_ref[...]
                tw = jnp.concatenate(
                    [(re * ct + im * st).astype(jnp.bfloat16), (im * ct - re * st).astype(jnp.bfloat16)],
                    axis=1,
                )
                sp = lax.dot_general(
                    tb_ref[...], tw, (((1,), (1,)), ((), ())), preferred_element_type=jnp.float32
                )
                for f in range(2):
                    gbuf[pl.ds(4 * g + 2 * u + f, rc, stride=frames), :] = sp[f * rc : (f + 1) * rc]

        def pack(j, total):
            for ri in range(2):
                for cc in range(cb):
                    at = pl.multiple_of((ri * half_c + j * cb + cc) * frames, frames)
                    tile = gbuf[pl.ds(at, frames), :].astype(jnp.bfloat16)
                    spec[s, j, ri, :, pl.ds(cc * LANES, LANES)] = tile
                    wide = tile.astype(jnp.float32)
                    total = total + wide * wide
            return total

        total = lax.fori_loop(0, n, pack, jnp.zeros((frames, LANES), jnp.float32))
        pall[s, me] = jnp.sum(total, axis=0, keepdims=True)

        def send(peer):
            pltpu.make_async_remote_copy(
                src_ref=pall.at[s, me],
                dst_ref=pall.at[s, me],
                send_sem=pow_send.at[s],
                recv_sem=pow_recv.at[s],
                device_id={"tm": peer},
                device_id_type=MESH,
            ).start()
            pltpu.make_async_remote_copy(
                src_ref=spec.at[s, peer],
                dst_ref=recv.at[s, :, pl.ds(me * frames, frames), :],
                send_sem=spec_send.at[s],
                recv_sem=spec_recv.at[s],
                device_id={"tm": peer},
                device_id_type=MESH,
            ).start()

        @pl.loop(0, n // 2)
        def _(o):
            send((1 - me // (n // 2)) * (n // 2) + lax.rem(me + o, n // 2))

        @pl.loop(1, n // 2)
        def _(o):
            send(me // (n // 2) * (n // 2) + lax.rem(me + o, n // 2))

        pltpu.make_async_copy(
            spec.at[s, me], recv.at[s, :, pl.ds(me * frames, frames), :], own_sem.at[s]
        ).start()

    @pl.loop(0, streams)
    def _(s):
        others = spec.at[s, pl.ds(0, n - 1)]
        pltpu.make_async_copy(others, others, spec_recv.at[s]).wait()
        pltpu.make_async_copy(
            spec.at[s, me], recv.at[s, :, pl.ds(me * frames, frames), :], own_sem.at[s]
        ).wait()
        part = pall.at[s, pl.ds(0, n - 1)]
        pltpu.make_async_copy(part, part, pow_recv.at[s]).wait()
        power = jnp.sum(jnp.sum(pall[s], axis=0), axis=1, keepdims=True)
        g = 0.378 / jnp.sqrt(power / count + 1e-06)
        for ri in range(2):
            flipped = lax.dot_general(
                eye_ref[...], recv[s, ri], (((1,), (1,)), ((), ())), preferred_element_type=jnp.float32
            )
            scaled = jnp.clip(flipped * g, -1.0, 1.0)
            out_ref[s, ri] = scaled.astype(jnp.bfloat16)
        pltpu.make_async_copy(out_ref.at[s], out_hbm.at[s], out_sem.at[s]).start()

    @pl.loop(0, streams)
    def _(s):
        others = spec.at[s, pl.ds(0, n - 1)]
        pltpu.make_async_copy(others, others, spec_send.at[s]).wait()
        part = pall.at[s, pl.ds(0, n - 1)]
        pltpu.make_async_copy(part, part, pow_send.at[s]).wait()

    @pl.when(me < n - 1)
    def _():
        @pl.loop(0, streams)
        def _(s):
            halo_copy(s).wait_send()

    @pl.when(relays)
    def _():
        @pl.loop(0, half_s)
        def _(s):
            from_relay(s + half_s).wait_send()

    @pl.loop(0, streams)
    def _(s):
        pltpu.make_async_copy(out_ref.at[s], out_hbm.at[s], out_sem.at[s]).wait()


def on_device_kernel(samples, filter_taps):
    n = lax.axis_size("tm")
    streams = samples.shape[0]
    taps, fft_len = filter_taps.shape
    frames = samples.shape[1] // fft_len
    rows = fft_len // LANES
    col_len = fft_len // ROW_LEN
    channels = fft_len // 2
    ch = channels // n
    stage_a, cos_t, sin_t, stage_b = kernel_tables(ROW_LEN, col_len)
    eye = jnp.asarray(np.eye(ch), jnp.bfloat16)
    hbm = pl.BlockSpec(memory_space=pl.ANY)
    dma = pltpu.SemaphoreType.DMA
    return pl.pallas_call(
        functools.partial(body, n, float(frames * n * channels)),
        out_shape=jax.ShapeDtypeStruct((streams, 2, ch, frames * n), jnp.bfloat16),
        in_specs=[hbm] * 7,
        out_specs=hbm,
        scratch_shapes=[
            pltpu.VMEM(samples.shape, samples.dtype),
            pltpu.VMEM(filter_taps.shape, filter_taps.dtype),
            *[pltpu.VMEM(t.shape, t.dtype) for t in (stage_a, cos_t, sin_t, stage_b, eye)],
            pltpu.VMEM((streams, 2, ch, frames * n), jnp.bfloat16),
            pltpu.VMEM((streams // 2, taps - 1, rows, LANES), jnp.bfloat16),
            pltpu.VMEM((streams * frames * rows, LANES), jnp.float32),
            pltpu.VMEM((taps * rows, LANES), jnp.float32),
            pltpu.VMEM((streams, frames + taps - 1, rows, LANES), jnp.bfloat16),
            pltpu.VMEM((frames // 2, 2 * rows, LANES), jnp.bfloat16),
            pltpu.VMEM((col_len * frames, LANES), jnp.float32),
            pltpu.VMEM((streams, n, 2, frames, ch), jnp.bfloat16),
            pltpu.VMEM((streams, 2, frames * n, ch), jnp.bfloat16),
            pltpu.VMEM((streams, n, 1, LANES), jnp.float32),
            dma((streams,)), dma((streams,)), dma((streams,)), dma((streams,)), dma((streams,)),
            dma((streams,)), dma((streams,)),
            dma((streams // 2,)), dma((streams // 2,)), dma((X_PIECES,)), dma((6,)), dma((streams,)),
        ],
        compiler_params=pltpu.CompilerParams(
            collective_id=0, has_side_effects=True, vmem_limit_bytes=VMEM_MIB * 1024 * 1024
        ),
    )(samples, filter_taps, stage_a, cos_t, sin_t, stage_b, eye)


target_level = 0.378
epsilon = 1e-06


def shifted(value, axis, by):
    size = lax.axis_size(axis)
    pairs = [(i, i + by) for i in range(size) if 0 <= i + by < size]
    return lax.ppermute(value, axis, pairs)


def tables(row_len, col_len):
    fft_len = row_len * col_len
    rows_a = jnp.arange(row_len, dtype=jnp.int32)
    cols_b = jnp.arange(col_len, dtype=jnp.int32)
    half_c = jnp.arange(col_len // 2, dtype=jnp.int32)
    angle_a = (
        2.0 * jnp.pi / row_len * (rows_a[:, None] * rows_a[None, :] % row_len).astype(jnp.float32)
    )
    angle_t = (
        2.0 * jnp.pi / fft_len * (cols_b[:, None] * rows_a[None, :] % fft_len).astype(jnp.float32)
    )
    angle_b = (
        2.0 * jnp.pi / col_len * (cols_b[:, None] * half_c[None, :] % col_len).astype(jnp.float32)
    )
    return (
        jnp.cos(angle_a).astype(jnp.bfloat16),
        jnp.sin(angle_a).astype(jnp.bfloat16),
        jnp.cos(angle_t),
        jnp.sin(angle_t),
        jnp.cos(angle_b).astype(jnp.bfloat16),
        jnp.sin(angle_b).astype(jnp.bfloat16),
    )


def transform(filtered):
    streams, frames, fft_len = filtered.shape
    col_len = fft_len // ROW_LEN
    cos_a, sin_a, cos_t, sin_t, cos_b, sin_b = tables(ROW_LEN, col_len)
    blocks = filtered.reshape(streams, frames, ROW_LEN, col_len)
    first_re = jnp.einsum("sfab,ad->sfbd", blocks, cos_a, preferred_element_type=jnp.float32)
    first_im = -jnp.einsum("sfab,ad->sfbd", blocks, sin_a, preferred_element_type=jnp.float32)
    twisted_re = (first_re * cos_t + first_im * sin_t).astype(jnp.bfloat16)
    twisted_im = (first_im * cos_t - first_re * sin_t).astype(jnp.bfloat16)
    spec_re = jnp.einsum(
        "sfbd,bc->scdf", twisted_re, cos_b, preferred_element_type=jnp.float32
    ) + jnp.einsum("sfbd,bc->scdf", twisted_im, sin_b, preferred_element_type=jnp.float32)
    spec_im = jnp.einsum(
        "sfbd,bc->scdf", twisted_im, cos_b, preferred_element_type=jnp.float32
    ) - jnp.einsum("sfbd,bc->scdf", twisted_re, sin_b, preferred_element_type=jnp.float32)
    return (spec_re.reshape(streams, -1, frames), spec_im.reshape(streams, -1, frames))


def on_device(samples, filter_taps):
    streams = samples.shape[0]
    tap_count, fft_len = filter_taps.shape
    frames = samples.shape[1] // fft_len
    signal = samples.reshape(streams, frames, fft_len)
    history = shifted(signal[:, frames - (tap_count - 1) :, :], "tm", 1)
    extended = jnp.concatenate([history, signal], axis=1)
    weights = filter_taps.astype(jnp.float32)
    filtered = jnp.zeros((streams, frames, fft_len), jnp.float32)
    for tap_index in range(tap_count):
        offset = tap_count - 1 - tap_index
        filtered = filtered + weights[tap_index] * extended[:, offset : offset + frames].astype(
            jnp.float32
        )
    filtered = filtered.astype(jnp.bfloat16)
    spec_re, spec_im = transform(filtered)
    real_part = spec_re.astype(jnp.bfloat16)
    imag_part = spec_im.astype(jnp.bfloat16)
    real_wide = real_part.astype(jnp.float32)
    imag_wide = imag_part.astype(jnp.float32)
    local_power = jnp.sum(real_wide * real_wide + imag_wide * imag_wide, axis=(1, 2))
    total_power = lax.psum(local_power, "tm")
    count = frames * lax.axis_size("tm") * spec_re.shape[1]
    gain = target_level / jnp.sqrt(total_power / count + epsilon)
    scaled = jnp.stack(
        [
            jnp.clip(real_wide * gain[:, None, None], -1.0, 1.0),
            jnp.clip(imag_wide * gain[:, None, None], -1.0, 1.0),
        ],
        axis=1,
    ).astype(jnp.bfloat16)
    result = lax.all_to_all(scaled, "tm", split_axis=2, concat_axis=3, tiled=True)
    return result


def solution(mesh):
    tm = mesh.shape["tm"]

    def on_shard(samples, filter_taps):
        fft_len = filter_taps.shape[1]
        frames = samples.shape[1] // fft_len
        whole_tiles = (fft_len // 2) % (tm * LANES) == 0 and (frames * tm) % LANES == 0
        if whole_tiles and frames % 16 == 0 and fft_len == LANES * (LANES // 2) and tm % 2 == 0:
            return on_device_kernel(samples, filter_taps)
        return on_device(samples, filter_taps)

    return jax.shard_map(
        on_shard,
        mesh=mesh,
        in_specs=(P("grp", "tm"), P()),
        out_specs=P("grp", None, "tm", None),
        check_vma=False,
    )
```
